128 devices in a mesh: row: 8 (over z, core), col: 16 (over y, x).
Axes of the slice: x: 4, y: 4, z: 4, core: 2. Of those that a mesh axis runs over, the one named last changes fastest.
Arguments:
- inverse_interior: float32 [8, 16, 1536, 1536], P('row', 'col'), may hold values from -0.15625 to 0.15625
- coupling: float32 [8, 16, 1536, 1024], P('row', 'col'), may hold values from -1 to 1
- interface_block: float32 [8, 16, 1024, 1024], P('row', 'col'), may hold values from -6 to 6
- iface_ids: int32 [8, 16, 4], P('row', 'col'), may hold values from 0 to 15, as said below
- row_place: int32 [16], replicated, may hold values from 0 to 15, as said below
- col_place: int32 [16], replicated, may hold values from 0 to 15, as said below
Outputs:
- assembled: float32 [16, 256, 16, 256], P('row', None, 'col')
The draws below stay inside these ranges and needn't reach their ends.
Inputs may be any that keep to these rules, and one draw needn't show every extreme that they name: `row_place`: A permutation of the tile ids. `col_place`: a permutation of the tile ids; two ids whose values of row_place differ mod 8 have values of col_place that differ mod 16. `iface_ids`: the 4 ids of one subdomain have pairwise different row_place mod 8, hence pairwise different col_place mod 16.
All inputs are finite; a program needn't handle non-finite values.
Results may differ from the reference program's by a relative error of at most 0.0001.
Values sent between devices are 32-bit elements; how exact they have to be, the bound alone decides.
A program may use at most 192 MiB of HBM per device.

```python
import jax
import jax.numpy as jnp
from jax import lax

NG = 1024
TILE = 256
NI = 1536
OWN_R = 2
NB = 4
PROWS = 8
PCOLS = 16
NT = 16
OWN_C = 1


def layout(key):
    row_place = jax.random.permutation(jax.random.fold_in(key, 11), NT).astype(jnp.int32)
    position = jnp.arange(NT, dtype=jnp.int32)
    owner = row_place % PROWS
    scores = jax.random.permutation(jax.random.fold_in(key, 12), NT).astype(jnp.int32)
    same_owner = owner[:, None] == owner[None, :]
    ranking = jnp.sum(same_owner & (scores[None, :] < scores[:, None]), axis=1).astype(jnp.int32)
    spread = PCOLS // PROWS
    col_owner = owner * spread + ranking % spread
    col_place = (ranking // spread * PCOLS + col_owner).astype(jnp.int32)
    inverse = jnp.zeros((NT,), jnp.int32).at[row_place].set(position)
    devices = PROWS * PCOLS
    weights = jax.random.randint(jax.random.fold_in(key, 13), (devices, PROWS), 0, 1 << 20).astype(jnp.int32)
    weights = weights * PROWS + jnp.arange(PROWS, dtype=jnp.int32)[None, :]
    owners = jnp.argsort(weights, axis=1)[:, :NB].astype(jnp.int32)
    slot_draw = jax.random.randint(jax.random.fold_in(key, 14), (devices, NB), 0, OWN_R).astype(jnp.int32)
    global_ids = inverse[slot_draw * PROWS + owners].astype(jnp.int32)
    return (row_place, col_place, global_ids.reshape(PROWS, PCOLS, NB))


def draw_row_place(key, part):
    return layout(key)[0]


def draw_col_place(key, part):
    return layout(key)[1]


def draw_iface_ids(key, part):
    return layout(key)[2]


def level_of(stream_key, shape, shards, smallest, top_value):
    factor_of, own = 1.0, jax.random.fold_in(stream_key, 6)
    for dim, parts in shards:
        heights = jnp.exp(jax.random.uniform(jax.random.fold_in(own, dim), (parts,), jnp.float32, smallest / len(shards), top_value / len(shards)))
        factor_of = factor_of * jnp.repeat(heights, shape[dim] // parts).reshape([-1 if axis == dim else 1 for axis in range(len(shape))])
    return factor_of


def noise(key, extent, width, reach, split=(), kind=jnp.bfloat16):
    factor_of = level_of(key, extent, split, -0.22, 0.18) if split else 1.0
    values = jax.random.normal(key, extent, jnp.float32) * width * factor_of
    return jnp.minimum(jnp.maximum(values, -reach), reach).astype(kind)


def setup_inputs(seed: int = 0) -> dict:
    key_list = jax.random.split(jax.random.key(seed), 7)
    return {
        "inverse_interior": noise(key_list[0], (PROWS, PCOLS, NI, NI), NI ** -0.5, 0.15625, ((0, 8), (1, 16)), jnp.float32),
        "coupling": noise(key_list[1], (PROWS, PCOLS, NI, NG), 0.16, 1.0, ((0, 8), (1, 16)), jnp.float32),
        "interface_block": noise(key_list[2], (PROWS, PCOLS, NG, NG), 1.0, 6.0, ((0, 8), (1, 16)), jnp.float32),
        "iface_ids": draw_iface_ids(jax.random.fold_in(key_list[6], 71), 0),
        "row_place": draw_row_place(jax.random.fold_in(key_list[6], 71), 0),
        "col_place": draw_col_place(jax.random.fold_in(key_list[6], 71), 0),
    }


def reference(inverse_interior, coupling, interface_block, iface_ids, row_place, col_place):
    highest = lax.Precision.HIGHEST
    out_rows = ((row_place % PROWS) * OWN_R + row_place // PROWS).astype(jnp.int32)
    out_cols = ((col_place % PCOLS) * OWN_C + col_place // PCOLS).astype(jnp.int32)
    tile_count = NG // TILE
    devices = PROWS * PCOLS

    def absorb(accum, items):
        inverse, couple, block, global_ids = items
        solved = jnp.dot(inverse, couple, precision=highest, preferred_element_type=jnp.float32)
        product = lax.dot_general(couple, solved, (((0,), (0,)), ((), ())), precision=highest, preferred_element_type=jnp.float32)
        schur_block = block - product
        tile_grid = schur_block.reshape(tile_count, TILE, tile_count, TILE).transpose(0, 2, 1, 3)
        row_index = out_rows[global_ids]
        col_index = out_cols[global_ids]
        accum = accum.at[row_index[:, None], :, col_index[None, :], :].add(tile_grid)
        return accum, None

    items = (inverse_interior.reshape(devices, NI, NI), coupling.reshape(devices, NI, NG), interface_block.reshape(devices, NG, NG), iface_ids.reshape(devices, NB))
    initial = jnp.zeros((NT, TILE, NT, TILE), jnp.float32)
    accum, ignored = lax.scan(absorb, initial, items)
    return accum
```

```python
import functools

import jax
import jax.numpy as jnp
from jax import lax
from jax.experimental import pallas as pl
from jax.experimental.pallas import tpu as pltpu
from jax.sharding import PartitionSpec as P

TILE = 256
MESH = pl.DeviceIdType.MESH

ORDER = (
    (0, 1), (1, 0), (0, 3), (3, 0), (0, 2), (2, 0), (1, 1), (3, 3),
    (1, 3), (3, 1), (1, 2), (2, 1), (2, 3), (3, 2), (2, 2),
)
ROTATION = (0, 0, 0, 0)


def plane_of(r, z, y, x):
    return ((y, x, z), (z, y, x), (x, z, y))[r]


def chip_of(r, u, v, w):
    return ((w, u, v), (u, v, w), (v, w, u))[r]


def kernel(pieces, table, out, arrived0, arrived1, arrived2, arrived3, table_in, table_s, give, take, grid, moved, done, final, zero_sem,
           data_s, data_r, tab_s, tab_r, own_sem, sib_s, sib_r, mov_s, mov_r, fin_s, fin_r):
    row, col = lax.axis_index("row"), lax.axis_index("col")
    z, core = row // 2, row % 2
    y, x = col // 4, col % 4
    arrived = (arrived0, arrived1, arrived2, arrived3)
    chunks = range(len(ROTATION))
    rotations = sorted(set(ROTATION))

    def device(zz, yy, xx, cc=None):
        return (zz * 2 + (core if cc is None else cc), yy * 4 + xx)

    def member(r, du, dv, dw=0):
        u, v, w = plane_of(r, z, y, x)
        return device(*chip_of(r, (u + du) % 4, (v + dv) % 4, (w + dw) % 4))

    def place(r, du=0, dv=0):
        u, v, _ = plane_of(r, z, y, x)
        return ((u + du) % 4) * 4 + (v + dv) % 4

    sibling = device(z, y, x, 1 - core)

    offsets = set()
    for r in rotations:
        for du, dv in ORDER:
            offsets.add(chip_of(r, du, dv, 0))
        for dw in (1, 2, 3):
            offsets.add(chip_of(r, 0, 0, dw))
    offsets = sorted(offsets)
    barrier = pltpu.get_barrier_semaphore()
    for dz, dy, dx in offsets:
        pl.semaphore_signal(barrier, inc=1, device_id=device((z + dz) % 4, (y + dy) % 4, (x + dx) % 4),
                            device_id_type=MESH)
    pl.semaphore_signal(barrier, inc=1, device_id=sibling, device_id_type=MESH)

    for c in chunks:
        arrived[c][:, 4, :] = jnp.zeros((16, 5, 8, 128), jnp.float32)
        arrived[c][:, :, 4] = jnp.zeros((16, 5, 8, 128), jnp.float32)
    pl.semaphore_wait(barrier, len(offsets) + 1)

    waits = []
    table_copies, data_copies = {}, {}
    for n, r in enumerate(rotations):
        for k, (du, dv) in enumerate(ORDER):
            copy = pltpu.make_async_remote_copy(
                src_ref=table, dst_ref=table_in.at[n, place(r)], send_sem=tab_s.at[n, k],
                recv_sem=tab_r.at[n, k], device_id=member(r, du, dv), device_id_type=MESH)
            copy.start()
            table_copies[n, k] = copy
    for c in chunks:
        r = ROTATION[c]
        for k, (du, dv) in enumerate(ORDER):
            copy = pltpu.make_async_remote_copy(
                src_ref=pieces.at[c, place(r, du, dv)], dst_ref=arrived[c].at[place(r), pl.ds(0, 4), pl.ds(0, 4)],
                send_sem=data_s.at[c, k], recv_sem=data_r.at[c, k],
                device_id=member(r, du, dv), device_id_type=MESH)
            copy.start()
            data_copies[c, k] = copy
    own_copies = []
    for c in chunks:
        p = place(ROTATION[c])
        copy = pltpu.make_async_copy(pieces.at[c, p], arrived[c].at[p, pl.ds(0, 4), pl.ds(0, 4)], own_sem.at[c])
        copy.start()
        own_copies.append(copy)
    for n, r in enumerate(rotations):
        table_in[n, place(r)] = table[...]
    for n, r in enumerate(rotations):
        for k in range(15):
            table_copies[n, k].wait()
        copy = pltpu.make_async_copy(table_in.at[n], table_s.at[n], zero_sem)
        copy.start()
        copy.wait()

    sib_copies, mov_copies, fin_copies = {}, {}, {}

    def reduce(c, target, who):
        r = ROTATION[c]
        n = rotations.index(r)

        def body(zz, carry):
            first = zz * 4 + who * 2
            acc = [[None] * 16 for _ in range(2)]
            for s in range(16):
                ra = [table_s[n, s, 0, first + slot] for slot in range(2)]
                for j in range(16):
                    cb = table_s[n, s, 0, 16 + j]
                    for slot in range(2):
                        block = arrived[c][s, ra[slot], cb]
                        acc[slot][j] = block if s == 0 else acc[slot][j] + block
            for j in range(16):
                u, v, w = plane_of(r, zz, j // 4, j % 4)
                for slot in range(2):
                    target[c, w, u * 4 + v, slot] = acc[slot][j]
            return carry

        lax.fori_loop(0, 4, body, 0)

    def stage_reduce(c):
        for k in range(15):
            data_copies[c, k].wait_recv()
        own_copies[c].wait()
        reduce(c, give, 1 - core)
        copy = pltpu.make_async_remote_copy(
            src_ref=give.at[c], dst_ref=take.at[c], send_sem=sib_s.at[c], recv_sem=sib_r.at[c],
            device_id=sibling, device_id_type=MESH)
        copy.start()
        sib_copies[c] = copy
        reduce(c, grid, core)

    def stage_move(c):
        r = ROTATION[c]
        _, _, w = plane_of(r, z, y, x)
        sib_copies[c].wait_recv()
        for dw in (2, 1, 3, 0):
            there = (w + dw) % 4
            grid[c, there] = grid[c, there] + take[c, there]
            if dw:
                copy = pltpu.make_async_remote_copy(
                    src_ref=grid.at[c, there], dst_ref=moved.at[c, dw - 1], send_sem=mov_s.at[c, dw - 1],
                    recv_sem=mov_r.at[c, dw - 1], device_id=member(r, 0, 0, dw), device_id_type=MESH)
                copy.start()
                mov_copies[c, dw] = copy

    def stage_final(c):
        r = ROTATION[c]
        _, _, w = plane_of(r, z, y, x)
        h, q = c // 2, c % 2
        for dw in (1, 2, 3):
            mov_copies[c, dw].wait_recv()
        done[c] = grid[c, w] + moved[c, 0] + moved[c, 1] + moved[c, 2]
        p = place(r)
        rows = pl.ds(pl.multiple_of(q * 128 + p * 8, 8), 8)
        for k, (du, dv) in enumerate(ORDER):
            copy = pltpu.make_async_remote_copy(
                src_ref=done.at[c, place(r, du, dv)], dst_ref=final.at[:, rows, pl.ds(h * 128, 128)],
                send_sem=fin_s.at[c, k], recv_sem=fin_r.at[c, k],
                device_id=member(r, du, dv), device_id_type=MESH)
            copy.start()
            fin_copies[c, k] = copy
        final[:, rows, h * 128:(h + 1) * 128] = done[c, p]

    last = len(ROTATION) - 1
    for step in range(last + 3):
        if step <= last:
            stage_reduce(step)
        if 0 <= step - 1 <= last:
            stage_move(step - 1)
        if 0 <= step - 2 <= last:
            stage_final(step - 2)
    for c in chunks:
        for k in range(15):
            fin_copies[c, k].wait_recv()
    out[...] = final[...]
    for c in chunks:
        for k in range(15):
            data_copies[c, k].wait_send()
            fin_copies[c, k].wait_send()
        for dw in (1, 2, 3):
            mov_copies[c, dw].wait_send()
        sib_copies[c].wait_send()


def on_device(inverse_interior, coupling, interface_block, iface_ids, row_place, col_place):
    high = lax.Precision.HIGH
    solved = jnp.dot(inverse_interior[0, 0], coupling[0, 0], precision=high, preferred_element_type=jnp.float32)
    product = lax.dot_general(coupling[0, 0], solved, (((0,), (0,)), ((), ())), precision=high,
                              preferred_element_type=jnp.float32)
    schur = interface_block[0, 0] - product
    pieces = schur.reshape(4, 2, 16, 8, 4, 2, 128).transpose(5, 1, 2, 0, 4, 3, 6).reshape(4, 16, 4, 4, 8, 128)
    ids = iface_ids[0, 0]
    rowpos = (row_place % 8) * 2 + row_place // 8
    matches = ids[:, None] == jnp.arange(16, dtype=jnp.int32)[None, :]
    rows = jnp.sum(jnp.where(matches, rowpos[None, :], 0), axis=1)
    cols = jnp.sum(jnp.where(matches, col_place[None, :], 0), axis=1)
    lane = jnp.arange(128, dtype=jnp.int32)
    wanted = jnp.concatenate([rows, cols + 16]).astype(jnp.int32)
    value = jnp.tile(jnp.arange(4, dtype=jnp.int32), 2)
    hit = wanted[:, None] == lane[None, :]
    table = jnp.where(jnp.any(hit, axis=0), jnp.sum(jnp.where(hit, value[:, None], 0), axis=0), 4)[None, :]
    chunks, planes = len(ROTATION), len(set(ROTATION))
    f32 = jnp.float32
    vmem = pl.BlockSpec(memory_space=pltpu.VMEM)
    dma = pltpu.SemaphoreType.DMA
    out = pl.pallas_call(
        kernel,
        out_shape=jax.ShapeDtypeStruct((2, 256, 256), f32),
        in_specs=[pl.BlockSpec(memory_space=pl.ANY), vmem],
        out_specs=vmem,
        scratch_shapes=[
            *[pltpu.VMEM((16, 5, 5, 8, 128), f32)] * chunks,
            pltpu.VMEM((planes, 16, 1, 128), jnp.int32),
            pltpu.SMEM((planes, 16, 1, 128), jnp.int32),
            pltpu.VMEM((chunks, 4, 16, 2, 8, 128), f32),
            pltpu.VMEM((chunks, 4, 16, 2, 8, 128), f32),
            pltpu.VMEM((chunks, 4, 16, 2, 8, 128), f32),
            pltpu.VMEM((chunks, 3, 16, 2, 8, 128), f32),
            pltpu.VMEM((chunks, 16, 2, 8, 128), f32),
            pltpu.VMEM((2, 256, 256), f32),
            dma,
            dma((chunks, 15)), dma((chunks, 15)),
            dma((planes, 15)), dma((planes, 15)),
            dma((chunks,)),
            dma((chunks,)), dma((chunks,)),
            dma((chunks, 3)), dma((chunks, 3)),
            dma((chunks, 15)), dma((chunks, 15)),
        ],
        compiler_params=pltpu.CompilerParams(collective_id=0, has_side_effects=True, vmem_limit_bytes=48 * 2**20),
    )(pieces, table)
    return out[:, :, None, :]


def solution(mesh):
    return jax.shard_map(
        on_device,
        mesh=mesh,
        in_specs=(
            P("row", "col", None, None),
            P("row", "col", None, None),
            P("row", "col", None, None),
            P("row", "col", None),
            P(),
            P(),
        ),
        out_specs=P("row", None, "col", None),
        check_vma=False,
    )
```

```python
import functools

import jax
import jax.numpy as jnp
from jax import lax
from jax.experimental import pallas as pl
from jax.experimental.pallas import tpu as pltpu
from jax.sharding import PartitionSpec as P

TILE = 256
MESH = pl.DeviceIdType.MESH

ORDER = (
    (0, 1), (1, 0), (0, 3), (3, 0), (0, 2), (2, 0), (1, 1), (3, 3),
    (1, 3), (3, 1), (1, 2), (2, 1), (2, 3), (3, 2), (2, 2),
)
ROTATION = (0, 1, 2, 0)


def plane_of(r, z, y, x):
    return ((y, x, z), (z, y, x), (x, z, y))[r]


def chip_of(r, u, v, w):
    return ((w, u, v), (u, v, w), (v, w, u))[r]


def split(value):
    high = value.astype(jnp.bfloat16)
    return high, (value - high.astype(jnp.float32)).astype(jnp.bfloat16)


def product(left_high, left_low, right_high, right_low):
    def dot(left, right):
        return jnp.dot(left, right, preferred_element_type=jnp.float32)

    return dot(left_high, right_high) + (dot(left_high, right_low) + dot(left_low, right_high))


def kernel(inverse, coupling, block, ids, row_place, col_place, out,
           a_in, a_high, a_low, c_in, c_high, c_low, t_high, t_low, x_high, x_low, s_in, pieces, table,
           arrived0, arrived1, arrived2, arrived3, table_in, table_s, give, take, grid, moved, done, final,
           a_sem, c_sem, s_sem, zero_sem,
           data_s, data_r, tab_s, tab_r, own_sem, sib_s, sib_r, mov_s, mov_r, fin_s, fin_r):
    row, col = lax.axis_index("row"), lax.axis_index("col")
    z, core = row // 2, row % 2
    y, x = col // 4, col % 4
    arrived = (arrived0, arrived1, arrived2, arrived3)
    chunks = range(len(ROTATION))
    rotations = sorted(set(ROTATION))

    def device(zz, yy, xx, cc=None):
        return (zz * 2 + (core if cc is None else cc), yy * 4 + xx)

    def member(r, du, dv, dw=0):
        u, v, w = plane_of(r, z, y, x)
        return device(*chip_of(r, (u + du) % 4, (v + dv) % 4, (w + dw) % 4))

    def place(r, du=0, dv=0):
        u, v, _ = plane_of(r, z, y, x)
        return ((u + du) % 4) * 4 + (v + dv) % 4

    sibling = device(z, y, x, 1 - core)

    offsets = set()
    for r in rotations:
        for du, dv in ORDER:
            offsets.add(chip_of(r, du, dv, 0))
        for dw in (1, 2, 3):
            offsets.add(chip_of(r, 0, 0, dw))
    offsets = sorted(offsets)
    barrier = pltpu.get_barrier_semaphore()
    for dz, dy, dx in offsets:
        pl.semaphore_signal(barrier, inc=1, device_id=device((z + dz) % 4, (y + dy) % 4, (x + dx) % 4),
                            device_id_type=MESH)
    pl.semaphore_signal(barrier, inc=1, device_id=sibling, device_id_type=MESH)

    blocks, slots, depth = 6, a_in.shape[0], 256

    def load_a(m):
        return pltpu.make_async_copy(
            inverse.at[0, 0, pl.ds(m * depth, depth), :], a_in.at[m % slots], a_sem.at[m % slots])

    def load_c(h):
        return [pltpu.make_async_copy(
            coupling.at[0, 0, :, pl.ds(b * 256 + h * 128, 128)], c_in.at[:, pl.ds(b * 128, 128)], c_sem.at[h, b])
            for b in range(4)]

    def load_s(h):
        return [pltpu.make_async_copy(
            block.at[0, 0, :, pl.ds(b * 256 + h * 128, 128)], s_in.at[h, :, pl.ds(b * 128, 128)], s_sem.at[h, b])
            for b in range(4)]

    c_loads = {h: load_c(h) for h in range(2)}
    s_loads = {h: load_s(h) for h in range(2)}
    a_loads = [load_a(m) for m in range(blocks)]
    for copy in c_loads[0]:
        copy.start()
    for m in range(slots):
        a_loads[m].start()
    for copy in s_loads[0] + s_loads[1]:
        copy.start()

    lane = lax.broadcasted_iota(jnp.int32, (1, 128), 1)
    value = jnp.full((1, 128), 4, jnp.int32)
    for k in range(4):
        g = ids[0, 0, k]
        rp, cp = row_place[g], col_place[g]
        value = jnp.where(lane == (rp & 7) * 2 + (rp >> 3), k, value)
        value = jnp.where(lane == 16 + (cp & 15) + (cp >> 4), k, value)
    table[...] = value
    for c in chunks:
        arrived[c][:, 4, :] = jnp.zeros((16, 5, 8, 128), jnp.float32)
        arrived[c][:, :, 4] = jnp.zeros((16, 5, 8, 128), jnp.float32)

    table_copies, data_copies = {}, {}

    def send(c):
        r = ROTATION[c]
        for k, (du, dv) in enumerate(ORDER):
            copy = pltpu.make_async_remote_copy(
                src_ref=pieces.at[c, place(r, du, dv)], dst_ref=arrived[c].at[place(r), pl.ds(0, 4), pl.ds(0, 4)],
                send_sem=data_s.at[c, k], recv_sem=data_r.at[c, k],
                device_id=member(r, du, dv), device_id_type=MESH)
            copy.start()
            data_copies[c, k] = copy
        p = place(r)
        copy = pltpu.make_async_copy(pieces.at[c, p], arrived[c].at[p, pl.ds(0, 4), pl.ds(0, 4)], own_sem.at[c])
        copy.start()
        own_copies[c] = copy

    def prepare_c(h):
        for copy in c_loads[h]:
            copy.wait()

        def body(n, carry):
            rows = pl.ds(pl.multiple_of(n * 128, 128), 128)
            value = c_in[rows, :]
            c_high[h, rows, :], c_low[h, rows, :] = split(value)
            t_high[h, :, rows], t_low[h, :, rows] = split(value.T)
            return carry

        lax.fori_loop(0, 12, body, 0)

    def solve(h, m):
        rows = pl.ds(m * depth, depth)
        if h == 0:
            a_loads[m].wait()
            a_high[rows, :], a_low[rows, :] = split(a_in[m % slots])
            if m + slots < blocks:
                a_loads[m + slots].start()

        def body(n, carry):
            cols = pl.ds(pl.multiple_of(n * 256, 256), 256)
            x_high[rows, cols], x_low[rows, cols] = split(
                product(a_high[rows, :], a_low[rows, :], c_high[h, :, cols], c_low[h, :, cols]))
            return carry

        lax.fori_loop(0, 2, body, 0)

    def finish(h, q):
        c = h * 2 + q

        def body(n, carry):
            cols = pl.ds(pl.multiple_of(n * 256, 256), 256)
            value = product(t_high[q], t_low[q], x_high[:, cols], x_low[:, cols])
            for a in range(4):
                for b in range(2):
                    mine = s_in[h, a * 256 + q * 128:a * 256 + q * 128 + 128,
                                pl.ds(pl.multiple_of(n * 256 + b * 128, 128), 128)]
                    tile = mine - value[a * 128:(a + 1) * 128, b * 128:(b + 1) * 128]
                    pieces[c, :, a, n * 2 + b] = tile.reshape(16, 8, 128)
            return carry

        lax.fori_loop(0, 2, body, 0)

    own_copies = {}
    prepare_c(0)
    for copy in c_loads[1]:
        copy.start()
    for m in range(blocks):
        solve(0, m)
    for copy in s_loads[0]:
        copy.wait()
    pl.semaphore_wait(barrier, len(offsets) + 1)
    finish(0, 0)
    send(0)
    for n, r in enumerate(rotations):
        for k, (du, dv) in enumerate(ORDER):
            copy = pltpu.make_async_remote_copy(
                src_ref=table, dst_ref=table_in.at[n, place(r)], send_sem=tab_s.at[n, k],
                recv_sem=tab_r.at[n, k], device_id=member(r, du, dv), device_id_type=MESH)
            copy.start()
            table_copies[n, k] = copy
    prepare_c(1)
    finish(0, 1)
    send(1)
    for m in range(blocks):
        solve(1, m)
    for copy in s_loads[1]:
        copy.wait()
    finish(1, 0)
    send(2)
    finish(1, 1)
    send(3)
    for n, r in enumerate(rotations):
        table_in[n, place(r)] = table[...]
    for n, r in enumerate(rotations):
        for k in range(15):
            table_copies[n, k].wait()
        copy = pltpu.make_async_copy(table_in.at[n], table_s.at[n], zero_sem)
        copy.start()
        copy.wait()

    sib_copies, mov_copies, fin_copies = {}, {}, {}

    def reduce(c, target, who):
        r = ROTATION[c]
        n = rotations.index(r)

        def body(zz, carry):
            first = zz * 4 + who * 2
            acc = [[None] * 16 for _ in range(2)]
            for s in range(16):
                ra = [table_s[n, s, 0, first + slot] for slot in range(2)]
                for j in range(16):
                    cb = table_s[n, s, 0, 16 + j]
                    for slot in range(2):
                        block = arrived[c][s, ra[slot], cb]
                        acc[slot][j] = block if s == 0 else acc[slot][j] + block
            for j in range(16):
                u, v, w = plane_of(r, zz, j // 4, j % 4)
                for slot in range(2):
                    target[c, w, u * 4 + v, slot] = acc[slot][j]
            return carry

        lax.fori_loop(0, 4, body, 0)

    def stage_reduce(c):
        for k in range(15):
            data_copies[c, k].wait_recv()
        own_copies[c].wait()
        reduce(c, give, 1 - core)
        copy = pltpu.make_async_remote_copy(
            src_ref=give.at[c], dst_ref=take.at[c], send_sem=sib_s.at[c], recv_sem=sib_r.at[c],
            device_id=sibling, device_id_type=MESH)
        copy.start()
        sib_copies[c] = copy
        reduce(c, grid, core)

    def stage_move(c):
        r = ROTATION[c]
        _, _, w = plane_of(r, z, y, x)
        sib_copies[c].wait_recv()
        for dw in (2, 1, 3, 0):
            there = (w + dw) % 4
            grid[c, there] = grid[c, there] + take[c, there]
            if dw:
                copy = pltpu.make_async_remote_copy(
                    src_ref=grid.at[c, there], dst_ref=moved.at[c, dw - 1], send_sem=mov_s.at[c, dw - 1],
                    recv_sem=mov_r.at[c, dw - 1], device_id=member(r, 0, 0, dw), device_id_type=MESH)
                copy.start()
                mov_copies[c, dw] = copy

    def stage_final(c):
        r = ROTATION[c]
        _, _, w = plane_of(r, z, y, x)
        h, q = c // 2, c % 2
        for dw in (1, 2, 3):
            mov_copies[c, dw].wait_recv()
        done[c] = grid[c, w] + moved[c, 0] + moved[c, 1] + moved[c, 2]
        p = place(r)
        rows = pl.ds(pl.multiple_of(q * 128 + p * 8, 8), 8)
        for k, (du, dv) in enumerate(ORDER):
            copy = pltpu.make_async_remote_copy(
                src_ref=done.at[c, place(r, du, dv)], dst_ref=final.at[:, rows, pl.ds(h * 128, 128)],
                send_sem=fin_s.at[c, k], recv_sem=fin_r.at[c, k],
                device_id=member(r, du, dv), device_id_type=MESH)
            copy.start()
            fin_copies[c, k] = copy
        final[:, rows, h * 128:(h + 1) * 128] = done[c, p]

    last = len(ROTATION) - 1
    for step in range(last + 3):
        if step <= last:
            stage_reduce(step)
        if 0 <= step - 1 <= last:
            stage_move(step - 1)
        if 0 <= step - 2 <= last:
            stage_final(step - 2)
    for c in chunks:
        for k in range(15):
            fin_copies[c, k].wait_recv()
    out[...] = final[...]
    for c in chunks:
        for k in range(15):
            data_copies[c, k].wait_send()
            fin_copies[c, k].wait_send()
        for dw in (1, 2, 3):
            mov_copies[c, dw].wait_send()
        sib_copies[c].wait_send()


def on_device(inverse_interior, coupling, interface_block, iface_ids, row_place, col_place):
    chunks, planes = len(ROTATION), len(set(ROTATION))
    f32, bf16 = jnp.float32, jnp.bfloat16
    vmem = pl.BlockSpec(memory_space=pltpu.VMEM)
    dma = pltpu.SemaphoreType.DMA
    out = pl.pallas_call(
        kernel,
        out_shape=jax.ShapeDtypeStruct((2, 256, 256), f32),
        in_specs=[pl.BlockSpec(memory_space=pl.ANY)] * 3 + [pl.BlockSpec(memory_space=pltpu.SMEM)] * 3,
        out_specs=vmem,
        scratch_shapes=[
            pltpu.VMEM((4, 256, 1536), f32),
            *[pltpu.VMEM((1536, 1536), bf16)] * 2,
            pltpu.VMEM((1536, 512), f32),
            *[pltpu.VMEM((2, 1536, 512), bf16)] * 2,
            *[pltpu.VMEM((2, 512, 1536), bf16)] * 2,
            *[pltpu.VMEM((1536, 512), bf16)] * 2,
            pltpu.VMEM((2, 1024, 512), f32),
            pltpu.VMEM((chunks, 16, 4, 4, 8, 128), f32),
            pltpu.VMEM((1, 128), jnp.int32),
            *[pltpu.VMEM((16, 5, 5, 8, 128), f32)] * chunks,
            pltpu.VMEM((planes, 16, 1, 128), jnp.int32),
            pltpu.SMEM((planes, 16, 1, 128), jnp.int32),
            pltpu.VMEM((chunks, 4, 16, 2, 8, 128), f32),
            pltpu.VMEM((chunks, 4, 16, 2, 8, 128), f32),
            pltpu.VMEM((chunks, 4, 16, 2, 8, 128), f32),
            pltpu.VMEM((chunks, 3, 16, 2, 8, 128), f32),
            pltpu.VMEM((chunks, 16, 2, 8, 128), f32),
            pltpu.VMEM((2, 256, 256), f32),
            dma((4,)), dma((2, 4)), dma((2, 4)), dma,
            dma((chunks, 15)), dma((chunks, 15)),
            dma((planes, 15)), dma((planes, 15)),
            dma((chunks,)),
            dma((chunks,)), dma((chunks,)),
            dma((chunks, 3)), dma((chunks, 3)),
            dma((chunks, 15)), dma((chunks, 15)),
        ],
        compiler_params=pltpu.CompilerParams(collective_id=0, has_side_effects=True, vmem_limit_bytes=60 * 2**20),
    )(inverse_interior, coupling, interface_block, iface_ids, row_place, col_place)
    return out[:, :, None, :]


def solution(mesh):
    return jax.shard_map(
        on_device,
        mesh=mesh,
        in_specs=(
            P("row", "col", None, None),
            P("row", "col", None, None),
            P("row", "col", None, None),
            P("row", "col", None),
            P(),
            P(),
        ),
        out_specs=P("row", None, "col", None),
        check_vma=False,
    )
```

```python
import functools

import jax
import jax.numpy as jnp
from jax import lax
from jax.experimental import pallas as pl
from jax.experimental.pallas import tpu as pltpu
from jax.sharding import PartitionSpec as P

TILE = 256
MESH = pl.DeviceIdType.MESH

ORDER = (
    (0, 1), (1, 0), (0, 3), (3, 0), (0, 2), (2, 0), (1, 1), (3, 3),
    (1, 3), (3, 1), (1, 2), (2, 1), (2, 3), (3, 2), (2, 2),
)
ROTATION = (0, 0, 0, 0)


def plane_of(r, z, y, x):
    return ((y, x, z), (z, y, x), (x, z, y))[r]


def chip_of(r, u, v, w):
    return ((w, u, v), (u, v, w), (v, w, u))[r]


STRIDE = 33


def split(value):
    high = value.astype(jnp.bfloat16)
    return high, (value - high.astype(jnp.float32)).astype(jnp.bfloat16)


def product(left_high, left_low, right_high, right_low):
    def dot(left, right):
        return jnp.dot(left, right, preferred_element_type=jnp.float32)

    return dot(left_high, right_high) + (dot(left_high, right_low) + dot(left_low, right_high))


def kernel(inverse, coupling, block, ids, row_place, col_place, out,
           a_in, a_high, a_low, c_in, c_high, c_low, t_high, t_low, x_high, x_low, s_in, pieces, table,
           arrived0, arrived1, arrived2, arrived3, table_in, table_s, give, take, grid, moved, done, final,
           a_sem, c_sem, s_sem, lab_sem,
           data_s, data_r, tab_s, tab_r, own_sem, sib_s, sib_r, mov_s, mov_r, fin_s, fin_r):
    row, col = lax.axis_index("row"), lax.axis_index("col")
    z, core = row // 2, row % 2
    y, x = col // 4, col % 4
    arrived = (arrived0, arrived1, arrived2, arrived3)
    chunks = range(len(ROTATION))
    rotations = sorted(set(ROTATION))

    def device(zz, yy, xx, cc=None):
        return (zz * 2 + (core if cc is None else cc), yy * 4 + xx)

    def member(r, du, dv, dw=0):
        u, v, w = plane_of(r, z, y, x)
        return device(*chip_of(r, (u + du) % 4, (v + dv) % 4, (w + dw) % 4))

    def place(r, du=0, dv=0):
        u, v, _ = plane_of(r, z, y, x)
        return ((u + du) % 4) * 4 + (v + dv) % 4

    sibling = device(z, y, x, 1 - core)
    blocks, slots, depth = 6, a_in.shape[0], 256

    def load_a(m):
        return pltpu.make_async_copy(
            inverse.at[0, 0, pl.ds(m * depth, depth), :], a_in.at[m % slots], a_sem.at[m % slots])

    def load_c(h, b):
        return pltpu.make_async_copy(
            coupling.at[0, 0, :, pl.ds(b * 256 + h * 128, 128)], c_in.at[h, :, pl.ds(b * 128, 128)], c_sem.at[h, b])

    def load_s(h, b):
        return pltpu.make_async_copy(
            block.at[0, 0, :, pl.ds(b * 256 + h * 128, 128)], s_in.at[h, :, pl.ds(b * 128, 128)], s_sem.at[h, b])

    a_loads = [load_a(m) for m in range(blocks)]
    c_loads = [[load_c(h, b) for b in range(4)] for h in range(2)]
    s_loads = [[load_s(h, b) for b in range(4)] for h in range(2)]
    for copy in c_loads[0]:
        copy.start()
    for m in range(slots):
        a_loads[m].start()

    offsets = set()
    for r in rotations:
        for du, dv in ORDER:
            offsets.add(chip_of(r, du, dv, 0))
        for dw in (1, 2, 3):
            offsets.add(chip_of(r, 0, 0, dw))
    offsets = sorted(offsets)
    barrier = pltpu.get_barrier_semaphore()
    for dz, dy, dx in offsets:
        pl.semaphore_signal(barrier, inc=1, device_id=device((z + dz) % 4, (y + dy) % 4, (x + dx) % 4),
                            device_id_type=MESH)
    pl.semaphore_signal(barrier, inc=1, device_id=sibling, device_id_type=MESH)

    lane = lax.broadcasted_iota(jnp.int32, (1, 128), 1)
    value = jnp.full((1, 128), 16, jnp.int32)
    for k in range(4):
        g = ids[0, 0, k]
        rp, cp = row_place[g], col_place[g]
        value = jnp.where(lane == (rp & 7) * 2 + (rp >> 3), k * 2, value)
        value = jnp.where(lane == 16 + (cp & 15) + (cp >> 4), (k // 2) * 8 + k % 2, value)
    table[...] = value
    for c in chunks:
        for n in range(16):
            arrived[c][n * STRIDE + 16:(n + 1) * STRIDE] = jnp.zeros((STRIDE - 16, 8, 128), jnp.float32)

    def prepare_c(h):
        for copy in c_loads[h]:
            copy.wait()

        def body(n, carry):
            rows = pl.ds(pl.multiple_of(n * 128, 128), 128)
            value = c_in[h, rows, :]
            c_high[h, rows, :], c_low[h, rows, :] = split(value)
            t_high[h, :, rows], t_low[h, :, rows] = split(value.T)
            return carry

        lax.fori_loop(0, 12, body, 0)

    def solve_first(m):
        rows = pl.ds(m * depth, depth)
        a_loads[m].wait()
        a_high[rows, :], a_low[rows, :] = split(a_in[m % slots])
        if m + slots < blocks:
            a_loads[m + slots].start()
        x_high[0, rows, :], x_low[0, rows, :] = split(
            product(a_high[rows, :], a_low[rows, :], c_high[0, :, 0:256], c_low[0, :, 0:256]))

    def solve(h, pair):
        cols = slice(pair * 256, pair * 256 + 256)

        def body(m, carry):
            rows = pl.ds(pl.multiple_of(m * 512, 512), 512)
            x_high[pair, rows, :], x_low[pair, rows, :] = split(
                product(a_high[rows, :], a_low[rows, :], c_high[h, :, cols], c_low[h, :, cols]))
            return carry

        lax.fori_loop(0, 3, body, 0)

    def finish(h, pair, q):
        value = product(t_high[q], t_low[q], x_high[pair], x_low[pair])
        for a in range(4):
            for b in range(2):
                mine = s_in[h, a * 256 + q * 128:a * 256 + q * 128 + 128,
                            pair * 256 + b * 128:pair * 256 + b * 128 + 128]
                tile = mine - value[a * 128:(a + 1) * 128, b * 128:(b + 1) * 128]
                pieces[h * 2 + q, :, pair * 8 + a * 2 + b] = tile.reshape(16, 8, 128)

    table_copies, data_copies, own_copies = {}, {}, {}

    def parts(c):
        return (0, 1) if c < 2 else (2,)

    def send(h, part, q):
        c = h * 2 + q
        r = ROTATION[c]
        p = place(r)
        start, size = (0, 16) if part == 2 else (part * 8, 8)
        target = arrived[c].at[pl.ds(p * STRIDE + start, size)]
        for k, (du, dv) in enumerate(ORDER):
            copy = pltpu.make_async_remote_copy(
                src_ref=pieces.at[c, place(r, du, dv), pl.ds(start, size)], dst_ref=target,
                send_sem=data_s.at[c, part % 2, k], recv_sem=data_r.at[c, part % 2, k],
                device_id=member(r, du, dv), device_id_type=MESH)
            copy.start()
            data_copies[c, part, k] = copy
        copy = pltpu.make_async_copy(pieces.at[c, p, pl.ds(start, size)], target, own_sem.at[c, part % 2])
        copy.start()
        own_copies[c, part] = copy

    def send_tables():
        for n, r in enumerate(rotations):
            for k, (du, dv) in enumerate(ORDER):
                copy = pltpu.make_async_remote_copy(
                    src_ref=table, dst_ref=table_in.at[n, place(r)], send_sem=tab_s.at[n, k],
                    recv_sem=tab_r.at[n, k], device_id=member(r, du, dv), device_id_type=MESH)
                copy.start()
                table_copies[n, k] = copy
            table_in[n, place(r)] = table[...]

    prepare_c(0)
    for m in range(blocks):
        solve_first(m)
        if m == 1:
            for copy in s_loads[0] + c_loads[1] + s_loads[1]:
                copy.start()
        if m == 3:
            pl.semaphore_wait(barrier, len(offsets) + 1)
            send_tables()
    for copy in s_loads[0]:
        copy.wait()
    finish(0, 0, 0)
    send(0, 0, 0)
    prepare_c(1)
    finish(0, 0, 1)
    send(0, 0, 1)
    solve(0, 1)
    finish(0, 1, 0)
    send(0, 1, 0)
    finish(0, 1, 1)
    send(0, 1, 1)
    for copy in s_loads[1]:
        copy.wait()
    for pair in range(2):
        solve(1, pair)
    for q in range(2):
        for pair in range(2):
            finish(1, pair, q)
        send(1, 2, q)

    for copy in table_copies.values():
        copy.wait()
    copy = pltpu.make_async_copy(table_in, table_s, lab_sem)
    copy.start()
    copy.wait()

    fin_copies = {}

    def total(c, zz, who):
        first = zz * 4 + who * 2
        acc = [[None] * 16 for _ in range(2)]
        for s in range(16):
            ra = [table_s[0, s, 0, first + slot] for slot in range(2)]
            for j in range(16):
                cb = table_s[0, s, 0, 16 + j]
                for slot in range(2):
                    piece = arrived[c][ra[slot] + cb + s * STRIDE]
                    acc[slot][j] = piece if s == 0 else acc[slot][j] + piece
        return acc

    def sib_copy(c, zz):
        return pltpu.make_async_remote_copy(
            src_ref=give.at[c, zz], dst_ref=take.at[c, zz], send_sem=sib_s.at[c, zz], recv_sem=sib_r.at[c, zz],
            device_id=sibling, device_id_type=MESH)

    def mov_copy(c, dw):
        there = (z + dw) % 4
        return pltpu.make_async_remote_copy(
            src_ref=grid.at[c, there], dst_ref=moved.at[c, dw - 1], send_sem=mov_s.at[c, dw - 1],
            recv_sem=mov_r.at[c, dw - 1], device_id=device(there, y, x), device_id_type=MESH)

    def stage_reduce(c):
        for part in parts(c):
            for k in range(15):
                data_copies[c, part, k].wait_recv()
            own_copies[c, part].wait()

        def other(n, carry):
            zz = (z + 3 - n) % 4
            acc = total(c, zz, 1 - core)
            for j in range(16):
                for slot in range(2):
                    give[c, zz, j, slot] = acc[slot][j]
            sib_copy(c, zz).start()
            return carry

        def mine(n, carry):
            zz = (z + 3 - n) % 4
            acc = total(c, zz, core)
            sib_copy(c, zz).wait_recv()
            for j in range(16):
                for slot in range(2):
                    grid[c, zz, j, slot] = acc[slot][j] + take[c, zz, j, slot]

            @pl.when(n < 3)
            def _():
                mov_copy(c, 3 - n).start()

            return carry

        lax.fori_loop(0, 4, other, 0)
        lax.fori_loop(0, 4, mine, 0)

    def stage_final(c):
        r = ROTATION[c]
        _, _, w = plane_of(r, z, y, x)
        h, q = c // 2, c % 2
        for dw in (1, 2, 3):
            mov_copy(c, dw).wait_recv()
        done[c] = grid[c, w] + moved[c, 0] + moved[c, 1] + moved[c, 2]
        p = place(r)
        rows = pl.ds(pl.multiple_of(q * 128 + p * 8, 8), 8)
        for k, (du, dv) in enumerate(ORDER):
            copy = pltpu.make_async_remote_copy(
                src_ref=done.at[c, place(r, du, dv)], dst_ref=final.at[:, rows, pl.ds(h * 128, 128)],
                send_sem=fin_s.at[c, k], recv_sem=fin_r.at[c, k],
                device_id=member(r, du, dv), device_id_type=MESH)
            copy.start()
            fin_copies[c, k] = copy
        final[:, rows, h * 128:(h + 1) * 128] = done[c, p]

    last = len(ROTATION) - 1
    for step in range(last + 2):
        if step <= last:
            stage_reduce(step)
    for c in chunks:
        stage_final(c)
    for c in chunks:
        for k in range(15):
            fin_copies[c, k].wait_recv()
    out[...] = final[...]
    for c in chunks:
        for k in range(15):
            for part in parts(c):
                data_copies[c, part, k].wait_send()
            fin_copies[c, k].wait_send()
        for dw in (1, 2, 3):
            mov_copy(c, dw).wait_send()
        for zz in range(4):
            sib_copy(c, zz).wait_send()


def on_device(inverse_interior, coupling, interface_block, iface_ids, row_place, col_place):
    chunks, planes = len(ROTATION), len(set(ROTATION))
    f32, bf16 = jnp.float32, jnp.bfloat16
    vmem = pl.BlockSpec(memory_space=pltpu.VMEM)
    dma = pltpu.SemaphoreType.DMA
    out = pl.pallas_call(
        kernel,
        out_shape=jax.ShapeDtypeStruct((2, 256, 256), f32),
        in_specs=[pl.BlockSpec(memory_space=pl.ANY)] * 3 + [pl.BlockSpec(memory_space=pltpu.SMEM)] * 3,
        out_specs=vmem,
        scratch_shapes=[
            pltpu.VMEM((3, 256, 1536), f32),
            *[pltpu.VMEM((1536, 1536), bf16)] * 2,
            pltpu.VMEM((2, 1536, 512), f32),
            *[pltpu.VMEM((2, 1536, 512), bf16)] * 2,
            *[pltpu.VMEM((2, 512, 1536), bf16)] * 2,
            *[pltpu.VMEM((2, 1536, 256), bf16)] * 2,
            pltpu.VMEM((2, 1024, 512), f32),
            pltpu.VMEM((chunks, 16, 16, 8, 128), f32),
            pltpu.VMEM((1, 128), jnp.int32),
            *[pltpu.VMEM((16 * STRIDE, 8, 128), f32)] * chunks,
            pltpu.VMEM((planes, 16, 1, 128), jnp.int32),
            pltpu.SMEM((planes, 16, 1, 128), jnp.int32),
            pltpu.VMEM((chunks, 4, 16, 2, 8, 128), f32),
            pltpu.VMEM((chunks, 4, 16, 2, 8, 128), f32),
            pltpu.VMEM((chunks, 4, 16, 2, 8, 128), f32),
            pltpu.VMEM((chunks, 3, 16, 2, 8, 128), f32),
            pltpu.VMEM((chunks, 16, 2, 8, 128), f32),
            pltpu.VMEM((2, 256, 256), f32),
            dma((4,)), dma((2, 4)), dma((2, 4)), dma,
            dma((chunks, 2, 15)), dma((chunks, 2, 15)),
            dma((planes, 15)), dma((planes, 15)),
            dma((chunks, 2)),
            dma((chunks, 4)), dma((chunks, 4)),
            dma((chunks, 3)), dma((chunks, 3)),
            dma((chunks, 15)), dma((chunks, 15)),
        ],
        compiler_params=pltpu.CompilerParams(collective_id=0, has_side_effects=True, vmem_limit_bytes=62 * 2**20),
    )(inverse_interior, coupling, interface_block, iface_ids, row_place, col_place)
    return out[:, :, None, :]


def solution(mesh):
    return jax.shard_map(
        on_device,
        mesh=mesh,
        in_specs=(
            P("row", "col", None, None),
            P("row", "col", None, None),
            P("row", "col", None, None),
            P("row", "col", None),
            P(),
            P(),
        ),
        out_specs=P("row", None, "col", None),
        check_vma=False,
    )
```
